32 devices in a mesh: tok: 16 (over z, x, core), blk: 2 (over y).
Axes of the slice: x: 2, y: 2, z: 4, core: 2. Of those that a mesh axis runs over, the one named last changes fastest.
Arguments:
- activations: bfloat16 [2048, 7168], P('tok', 'blk'), may hold values from -600 to 600
- signs: float32 [7168], P('blk'), may hold values from -1 to 1, as said below
Outputs:
- hessian: float32 [7168, 7168], P('tok', 'blk')
- incoherence: float32 [7168], P('blk')
- largest_ratio: float32 [], replicated
The draws below stay inside these ranges and needn't reach their ends.
Inputs may be any that keep to these rules, and one draw needn't show every extreme that they name: `signs`: every entry is -1 or 1.
All inputs are finite; a program needn't handle non-finite values.
Results may differ from the reference program's by a relative error of at most 0.0037.
Values may be sent and summed in bfloat16 or wider, within the bound.
A program may use at most 640 MiB of HBM per device.

```python
import math
import jax
import jax.numpy as jnp
from jax import lax

WALSH = 512
MIX = 14
FEATURES = 7168
TOKENS = 2048


def draw_activations(key, part):
    noise_key, scale_key = jax.random.split(key, 2)
    position = jnp.arange(TOKENS, dtype=jnp.float32) / TOKENS
    ramp = jnp.exp(math.log(3.0) * position)[:, None]
    row_scale = jnp.exp(jax.random.uniform(scale_key, (TOKENS, 1), jnp.float32, 0.0, math.log(10.0)))
    values = jnp.clip(jax.random.normal(noise_key, (TOKENS, FEATURES), jnp.float32), -5.0, 5.0)
    return (values * ramp * row_scale).astype(jnp.bfloat16)


def draw_signs(key, part):
    coins = jax.random.randint(key, (FEATURES,), 0, 2)
    return (2 * coins - 1).astype(jnp.float32)


def setup_inputs(seed: int = 0) -> dict:
    seeds = jax.random.split(jax.random.key(seed), 3)
    return {
        "activations": draw_activations(jax.random.fold_in(seeds[2], 71), 0),
        "signs": draw_signs(jax.random.fold_in(seeds[2], 71), 0),
    }


EPS = 1e-06
DAMP = 0.01

def walsh_table(length):
    position = jnp.arange(length, dtype=jnp.int32)
    parity = jnp.zeros((length, length), jnp.int32)
    for bit_number in range(length.bit_length() - 1):
        parity = parity + (position[:, None] >> bit_number & 1) * (position[None, :] >> bit_number & 1)
    return (1 - 2 * (parity % 2)).astype(jnp.float32)

def cosine_table(length):
    rows_idx = jnp.arange(length, dtype=jnp.float32)[:, None]
    columns = jnp.arange(length, dtype=jnp.float32)[None, :]
    table = math.sqrt(2.0 / length) * jnp.cos(math.pi * (columns + 0.5) * rows_idx / length)
    return jnp.where(rows_idx == 0.0, table * math.sqrt(0.5), table)

def reference(activations, signs):
    signed = activations * signs.astype(jnp.bfloat16)[None, :]
    tokens_total = activations.shape[0]
    values = signed.astype(jnp.float32).reshape(tokens_total, WALSH, MIX)
    values = jnp.einsum('tba,ka->tbk', values, cosine_table(MIX), precision=lax.Precision.HIGHEST)
    values = jnp.einsum('tbk,cb->tck', values, walsh_table(WALSH) / math.sqrt(WALSH), precision=lax.Precision.HIGHEST)
    rotated = values.reshape(tokens_total, FEATURES).astype(jnp.bfloat16)
    gram_matrix = lax.dot_general(rotated, rotated, (((0,), (0,)), ((), ())), preferred_element_type=jnp.float32)
    on_diag = jnp.eye(FEATURES, dtype=jnp.bool_)
    trace_total = jnp.sum(jnp.diagonal(gram_matrix))
    diag_mean = trace_total / FEATURES + EPS
    hessian = gram_matrix / diag_mean + DAMP * on_diag.astype(jnp.float32)
    column_peak = lax.optimization_barrier(jnp.max(jnp.where(on_diag, 0.0, jnp.abs(gram_matrix)), axis=0))
    incoherence = column_peak / diag_mean
    return (hessian, incoherence, jnp.max(incoherence))
```

```python
import functools
import math

import jax
import jax.numpy as jnp
import numpy as np
from jax import lax
from jax.experimental import pallas as pl
from jax.experimental.pallas import tpu as pltpu
from jax.sharding import PartitionSpec as P

WALSH = 512
MIX = 14
FEATURES = 7168

EPS = 1e-06
DAMP = 0.01

LANES = 128
UNIT_WALSH = LANES // math.gcd(LANES, MIX)
UNIT = UNIT_WALSH * MIX
MESH = pl.DeviceIdType.MESH


def parity(number):
    return bin(number).count("1") & 1


def unit_tables():
    walsh = np.array(
        [[1 - 2 * parity(i & j) for j in range(UNIT_WALSH)] for i in range(UNIT_WALSH)], np.float64
    )
    k = np.arange(MIX)[:, None]
    n = np.arange(MIX)[None, :]
    cosine = math.sqrt(2.0 / MIX) * np.cos(math.pi * (n + 0.5) * k / MIX)
    cosine[0] *= math.sqrt(0.5)
    table = np.kron(walsh, cosine.T).astype(np.float32)
    high = table.astype(jnp.bfloat16)
    low = (table - high.astype(np.float32)).astype(jnp.bfloat16)
    return high, low


def bits_of(number, count):
    return [number // 2**j % 2 for j in range(count.bit_length() - 1)]


def swapped(me, k, count):
    total = 0
    for j, bit in enumerate(bits_of(me, count)):
        total += ((1 - bit) if k >> j & 1 else bit) * 2**j
    return total


def flip(me, k, count):
    odd = 0
    for j, bit in enumerate(bits_of(me, count)):
        odd += 0 if k >> j & 1 else bit
    return 1.0 if isinstance(odd, int) else (1 - 2 * (odd % 2)).astype(jnp.float32)


def place(tok, row_count, width, window):
    first = tok * row_count
    owner = first // width
    offset = first - owner * width
    start = jnp.minimum(offset // LANES * LANES, width - window)
    return owner, start, offset - start


def window_size(groups, row_count, width):
    need = max(i * row_count % width % LANES + row_count for i in range(groups))
    return min(-(-need // LANES) * LANES, width)


def tile_size(width):
    return max(t for t in range(LANES, 513, LANES) if width % t == 0)


def remote(src, dst, send, arrive, to_tok, to_blk):
    return pltpu.make_async_remote_copy(
        src, dst, send, arrive, device_id={"tok": to_tok, "blk": to_blk}, device_id_type=MESH
    )


def greet_all(tok, blk):
    tokens, blocks = lax.axis_size("tok"), lax.axis_size("blk")
    count = tokens * blocks
    barrier = pltpu.get_barrier_semaphore()
    me = tok * blocks + blk

    @pl.loop(1, count)
    def _(k):
        other = lax.rem(me + k, count)
        pl.semaphore_signal(
            barrier, inc=1, device_id={"tok": other // blocks, "blk": other % blocks}, device_id_type=MESH
        )

    pl.semaphore_wait(barrier, count - 1)


def broadcast_start(tok, blk, src, dst, send, recv):
    tokens, blocks = lax.axis_size("tok"), lax.axis_size("blk")
    count = tokens * blocks
    me = tok * blocks + blk

    @pl.loop(1, count)
    def _(k):
        other = lax.rem(me + k, count)
        remote(src, dst.at[me], send, recv, other // blocks, other % blocks).start()


def broadcast_wait(tok, blk, dst, send, recv):
    count = lax.axis_size("tok") * lax.axis_size("blk") - 1
    both = remote(dst.at[pl.ds(0, count)], dst.at[pl.ds(0, count)], send, recv, tok, blk)
    both.wait_send()
    both.wait_recv()


def kernel(
    depth, across, sub, early, lag, row_count, x_ref, signs_ref, high_hbm, low_hbm,
    hess_ref, ratio_ref, top_ref,
    cols, rows, pieces, signs, high, low, lhs, acc, left, square, parts, best, peaks,
    table_sem, x_sem, sign_sem, sign_send, sign_recv, swap_send, swap_recv,
    recv, pair_send, pair_recv, z_send, x_send, y_send, y_recv, part_send, part_recv, peak_send, peak_recv,
):
    tok, blk = lax.axis_index("tok"), lax.axis_index("blk")
    blocks, groups = lax.axis_size("blk"), lax.axis_size("tok")
    tok_rows, width = x_ref.shape
    window = rows.shape[1]
    half = cols.shape[0] // 2
    steps = tok_rows // sub
    chunks = width // UNIT
    core, chip = tok % 2, tok // 2
    z, x = chip // across, chip % across
    me = tok * blocks + blk
    owner, start, skew = place(tok, row_count, width, window)
    start = pl.multiple_of(start, LANES)

    loads = [
        pltpu.make_async_copy(high_hbm, high, table_sem.at[0]),
        pltpu.make_async_copy(low_hbm, low, table_sem.at[1]),
        pltpu.make_async_copy(x_ref, pieces.at[0], x_sem),
        pltpu.make_async_copy(signs_ref, signs.at[0], sign_sem),
    ]
    for load in loads:
        load.start()
    greet_all(tok, blk)

    for k in range(1, blocks):
        remote(signs_ref, signs.at[k], sign_send, sign_recv.at[k], tok, swapped(blk, k, blocks)).start()

    @pl.loop(0, steps)
    def _(s):
        piece = pl.ds(pl.multiple_of(s * sub, sub), sub)
        for k in range(1, blocks):
            remote(
                x_ref.at[piece], pieces.at[k, piece], swap_send, swap_recv.at[k * steps + s],
                tok, swapped(blk, k, blocks),
            ).start()

    for load in loads:
        load.wait()
    for k in range(1, blocks):
        remote(signs.at[k], signs.at[k], sign_send, sign_recv.at[k], tok, blk).wait_recv()
    square[...] = jnp.zeros_like(square)

    def first_row(oz, ox, s):
        return pl.multiple_of(((oz * across + ox) * 2 + core) * tok_rows + s * sub, sub)

    def rotate(s):
        piece = pl.ds(pl.multiple_of(s * sub, sub), sub)
        for k in range(1, blocks):
            landed = pieces.at[k, piece]
            remote(landed, landed, swap_send, swap_recv.at[k * steps + s], tok, blk).wait_recv()
        for k in range(blocks):
            for c in range(chunks):
                lanes = slice(c * UNIT, (c + 1) * UNIT)
                value = pieces[k, piece, lanes].astype(jnp.float32) * signs[k, :, lanes]
                first = (k * chunks + c) * sub
                lhs[first : first + sub, :] = value.astype(jnp.bfloat16)
        value = jnp.dot(lhs[...], high[...], preferred_element_type=jnp.float32)
        value += jnp.dot(lhs[...], low[...], preferred_element_type=jnp.float32)
        mixed = []
        for c in range(chunks):
            total = None
            for k in range(blocks):
                first = (k * chunks + c) * sub
                part = value[first : first + sub] * flip(blk, k, blocks)
                total = part if total is None else total + part
            mixed.append(total)
        step = 1
        while step < chunks:
            for a in range(chunks):
                if not a & step:
                    p, q = mixed[a], mixed[a | step]
                    mixed[a], mixed[a | step] = p + q, p - q
            step *= 2
        row = first_row(z, x, s)
        total = square[...]
        for c in range(chunks):
            rounded = (mixed[c] * (1.0 / math.sqrt(WALSH))).astype(jnp.bfloat16)
            cols[pl.ds(row, sub), c * UNIT : (c + 1) * UNIT] = rounded
            wide = rounded.astype(jnp.float32)
            wide = wide * wide
            for i in range(0, sub, 8):
                for j in range(0, UNIT, LANES):
                    total += wide[i : i + 8, j : j + LANES]
        square[...] = total

    def fan(oz, ox, s, z_ways, x_ways):
        row = first_row(oz, ox, s)
        src = cols.at[pl.ds(row, sub)]
        arrive = recv.at[(oz * across + ox) * steps + s]
        for way in z_ways:

            @pl.when((z + way >= 0) & (z + way < depth))
            def _():
                remote(src, src, z_send.at[(way + 1) // 2], arrive, tok + 2 * across * way, blk).start()

        for way in x_ways:

            @pl.when((x + way >= 0) & (x + way < across))
            def _():
                remote(src, src, x_send.at[(way + 1) // 2], arrive, tok + 2 * way, blk).start()

        remote(src, src, pair_send, pair_recv.at[oz * across + ox], tok + 1 - 2 * core, blk).start()
        for j in range(2):
            j_owner, j_start, _ = place(chip * 2 + j, row_count, width, window)

            @pl.when(j_owner == blk)
            def _():
                part = cols.at[pl.ds(row, sub), pl.ds(pl.multiple_of(j_start, LANES), window)]
                for k in range(1, blocks):
                    remote(
                        part, rows.at[pl.ds(row, sub)], y_send.at[2 * k + j],
                        y_recv.at[oz * across + ox], chip * 2 + j, lax.rem(blk + k, blocks),
                    ).start()

    def relay(oz, ox, s, z_ways, x_ways):
        piece = cols.at[pl.ds(first_row(oz, ox, s), sub)]
        remote(piece, piece, pair_send, recv.at[(oz * across + ox) * steps + s], tok, blk).wait_recv()
        fan(oz, ox, s, z_ways, x_ways)

    def inside(oz, ox):
        return (oz >= 0) & (oz < depth) & (ox >= 0) & (ox < across)

    def along_z(d, s):
        for way in (1, -1):
            oz = z - way * d

            @pl.when(inside(oz, x))
            def _():
                relay(oz, x, s, (way,), (1, -1))

    def along_x(d, dx, s):
        for side in (1, -1) if d else (1,):
            oz = z - side * d
            for way in (1, -1):
                ox = x - way * dx

                @pl.when(inside(oz, ox))
                def _():
                    relay(oz, ox, s, (), (way,))

    def early_x(dx, s):
        for way in (1, -1):
            ox = x - way * dx

            @pl.when(inside(z, ox))
            def _():
                relay(z, ox, s, (1, -1), (way,))

    def early_z(d):
        for way in (1, -1):
            oz = z - way * d

            @pl.when(inside(oz, x))
            def _():
                @pl.loop(0, across * early)
                def _(n):
                    relay(oz, n // early, n % early, (way,), ())

    tile = tile_size(width)

    def gram(stage):
        @pl.loop(0, depth * across)
        def _(n):
            oz, ox = n // across, n % across

            def away(a, b, d):
                return (a - b == d) | (b - a == d)

            due = (ox == x) & away(oz, z, stage)
            if stage:
                due = due | away(ox, x, 1) & away(oz, z, stage - 1)
            if stage == depth:
                for dx in range(2, across):
                    due = due | away(ox, x, dx)

            @pl.when(due)
            def _():
                chunk = pl.ds(pl.multiple_of(n * 2 * tok_rows, sub), 2 * tok_rows)
                piece = cols.at[pl.ds(0, tok_rows)]
                remote(piece, piece, pair_send, pair_recv.at[n], tok, blk).wait_recv()

                @pl.when(owner == blk)
                def _():
                    left[...] = jnp.transpose(cols[chunk, pl.ds(start, window)])

                @pl.when(owner != blk)
                def _():
                    piece = rows.at[pl.ds(0, 2 * tok_rows)]
                    remote(piece, piece, pair_send, y_recv.at[n], tok, blk).wait_recv()
                    left[...] = jnp.transpose(rows[chunk, :])

                @pl.loop(0, width // tile)
                def _(t):
                    lanes = pl.ds(pl.multiple_of(t * tile, tile), tile)
                    block = jnp.dot(left[...], cols[chunk, lanes], preferred_element_type=jnp.float32)
                    if stage:
                        acc[:, lanes] += block
                    else:
                        acc[:, lanes] = block

    @pl.loop(0, steps + lag)
    def _(s):
        @pl.when(s < steps)
        def _():
            rotate(s)
            fan(z, x, s, (1, -1), (1, -1))

        if depth * across > 1:

            @pl.when((s >= lag) & (s < lag + early))
            def _():
                for dx in range(1, across):
                    early_x(dx, s - lag)

            @pl.when(s >= lag + early)
            def _():
                along_z(1, s - lag)
                along_x(0, 1, s - lag)

    parts[me] = square[...]
    broadcast_start(tok, blk, square, parts, part_send, part_recv)
    gram(0)
    early_z(1)
    for d in range(2, depth):

        @pl.loop(early, steps)
        def _(s):
            along_z(d, s)
            along_x(d - 1, 1, s)

        early_z(d)
        gram(d - 1)

    @pl.loop(early, steps)
    def _(s):
        along_x(depth - 1, 1, s)

    for dx in range(2, across):
        for d in range(depth):

            @pl.loop(early, steps)
            def _(s):
                along_x(d, dx, s)

    gram(depth - 1)
    gram(depth)

    broadcast_wait(tok, blk, parts, part_send, part_recv)
    total = jnp.sum(jnp.sum(parts[...], axis=0), keepdims=True)
    inverse = 1.0 / (total / FEATURES + EPS)
    base = tok * row_count - blk * width

    best[...] = jnp.zeros_like(best)

    @pl.loop(0, width // tile)
    def _(t):
        lanes = pl.ds(pl.multiple_of(t * tile, tile), tile)
        row = lax.broadcasted_iota(jnp.int32, (window, tile), 0) + (base - skew - t * tile)
        column = lax.broadcasted_iota(jnp.int32, (window, tile), 1)
        size = jnp.where(row == column, 0.0, jnp.abs(acc[:, lanes]))
        most = best[...]
        for j in range(0, tile, LANES):
            most = jnp.maximum(most, size[:, j : j + LANES])
        best[...] = most

    flat = jnp.max(jnp.transpose(best[...]), axis=0, keepdims=True)
    lane = lax.broadcasted_iota(jnp.int32, (1, window), 1)
    flat = jnp.where((lane >= skew) & (lane < skew + row_count), flat, 0.0) * inverse
    peaks[me] = flat
    broadcast_start(tok, blk, peaks.at[me], peaks, peak_send, peak_recv)

    @pl.loop(0, width // tile)
    def _(t):
        lanes = pl.ds(pl.multiple_of(t * tile, tile), tile)
        row = lax.broadcasted_iota(jnp.int32, (row_count, tile), 0) + (base - t * tile)
        column = lax.broadcasted_iota(jnp.int32, (row_count, tile), 1)
        block = acc[pl.ds(pl.multiple_of(skew, 8), row_count), lanes]
        hess_ref[:, lanes] = block * inverse + jnp.where(row == column, DAMP, 0.0)

    def settle(count, send):
        piece = cols.at[pl.ds(0, count)]
        remote(piece, piece, send, part_recv, tok, blk).wait_send()

    late = steps - early
    for v in range(depth):

        @pl.when(z == v)
        def _():
            unit = (late + early * across) * sub
            if v < depth - 1:
                settle((v + 1) * unit, z_send.at[1])
            if v > 0:
                settle((depth - v) * unit, z_send.at[0])

    for v in range(across):

        @pl.when(x == v)
        def _():
            unit = (late * depth + early) * sub
            if v < across - 1:
                settle((v + 1) * unit, x_send.at[1])
            if v > 0:
                settle((across - v) * unit, x_send.at[0])

    settle(half, pair_send)
    for j in range(2):
        j_owner, _, _ = place(chip * 2 + j, row_count, width, window)

        @pl.when(j_owner == blk)
        def _():
            piece = rows.at[pl.ds(0, half)]
            for k in range(1, blocks):
                remote(piece, piece, y_send.at[2 * k + j], part_recv, tok, blk).wait_send()

    for k in range(1, blocks):
        remote(signs.at[k], signs.at[k], sign_send, part_recv, tok, blk).wait_send()
    if blocks > 1:
        sent = pieces.at[pl.ds(0, blocks - 1)]
        remote(sent, sent, swap_send, part_recv, tok, blk).wait_send()

    broadcast_wait(tok, blk, peaks, peak_send, peak_recv)
    most = peaks[0]
    for i in range(1, groups * blocks):
        most = jnp.maximum(most, peaks[i])
    top_ref[...] = jnp.broadcast_to(jnp.max(most, keepdims=True), top_ref.shape)
    for j in range(0, width, window):
        ratio_ref[:, j : j + window] = jnp.zeros((1, window), jnp.float32)
    for b in range(blocks):

        @pl.when(blk == b)
        def _():
            for i in range(groups):
                first = i * row_count
                if first // width == b:
                    offset = first % width
                    begin = min(offset // LANES * LANES, width - window)
                    most = ratio_ref[:, begin : begin + window]
                    for k in range(blocks):
                        most = jnp.maximum(most, peaks[i * blocks + k])
                    ratio_ref[:, begin : begin + window] = most


def per_device(activations, signs):
    tok_rows, width = activations.shape
    groups, blocks = lax.axis_size("tok"), lax.axis_size("blk")
    depth = 4 if groups % 8 == 0 else 1
    across = groups // (2 * depth)
    sub, early, lag = 16, 1, 2
    steps = tok_rows // sub
    row_count = FEATURES // groups
    window = window_size(groups, row_count, width)
    count, chips, tokens = groups * blocks, groups // 2, groups * tok_rows
    high, low = unit_tables()
    dma = pltpu.SemaphoreType.DMA
    anywhere = pl.BlockSpec(memory_space=pl.ANY)
    vmem = pl.BlockSpec(memory_space=pltpu.VMEM)
    hessian, ratio, top = pl.pallas_call(
        functools.partial(kernel, depth, across, sub, early, lag, row_count),
        out_shape=(
            jax.ShapeDtypeStruct((row_count, width), jnp.float32),
            jax.ShapeDtypeStruct((1, width + window), jnp.float32),
            jax.ShapeDtypeStruct((8, LANES), jnp.float32),
        ),
        in_specs=[anywhere] * 4,
        out_specs=(vmem, vmem, vmem),
        scratch_shapes=[
            pltpu.VMEM((tokens, width), jnp.bfloat16),
            pltpu.VMEM((tokens, window), jnp.bfloat16),
            pltpu.VMEM((blocks, tok_rows, width), jnp.bfloat16),
            pltpu.VMEM((blocks + 1, 1, width), jnp.float32),
            pltpu.VMEM((UNIT, UNIT), jnp.bfloat16),
            pltpu.VMEM((UNIT, UNIT), jnp.bfloat16),
            pltpu.VMEM((blocks * (width // UNIT) * sub, UNIT), jnp.bfloat16),
            pltpu.VMEM((window, width), jnp.float32),
            pltpu.VMEM((window, 2 * tok_rows), jnp.bfloat16),
            pltpu.VMEM((8, LANES), jnp.float32),
            pltpu.VMEM((count, 8, LANES), jnp.float32),
            pltpu.VMEM((window, LANES), jnp.float32),
            pltpu.VMEM((count + 1, 1, window), jnp.float32),
            dma((2,)), dma, dma, dma, dma((blocks,)), dma, dma((blocks * steps,)),
            dma((chips * steps,)), dma, dma((chips,)), dma((2,)), dma((2,)), dma((2 * blocks,)), dma((chips,)),
            dma, dma, dma, dma,
        ],
        compiler_params=pltpu.CompilerParams(
            collective_id=0, has_side_effects=True, vmem_limit_bytes=56 * 1024 * 1024
        ),
        name="fused",
    )(activations, signs.reshape(1, width), jnp.asarray(high), jnp.asarray(low))
    return hessian, ratio[0, :width], top[0, 0]


def solution(mesh):
    in_specs = (P("tok", "blk"), P("blk"))
    out_specs = (P("tok", "blk"), P("blk"), P())
    return jax.shard_map(
        per_device, mesh=mesh, in_specs=in_specs, out_specs=out_specs, check_vma=False
    )
```

```python
import functools
import math

import jax
import jax.numpy as jnp
import numpy as np
from jax import lax
from jax.experimental import pallas as pl
from jax.experimental.pallas import tpu as pltpu
from jax.sharding import PartitionSpec as P

WALSH = 512
MIX = 14
FEATURES = 7168

EPS = 1e-06
DAMP = 0.01

LANES = 128
UNIT_WALSH = LANES // math.gcd(LANES, MIX)
UNIT = UNIT_WALSH * MIX
MESH = pl.DeviceIdType.MESH


def parity(number):
    return bin(number).count("1") & 1


def unit_tables():
    walsh = np.array(
        [[1 - 2 * parity(i & j) for j in range(UNIT_WALSH)] for i in range(UNIT_WALSH)], np.float64
    )
    k = np.arange(MIX)[:, None]
    n = np.arange(MIX)[None, :]
    cosine = math.sqrt(2.0 / MIX) * np.cos(math.pi * (n + 0.5) * k / MIX)
    cosine[0] *= math.sqrt(0.5)
    table = np.kron(walsh, cosine.T).astype(np.float32)
    high = table.astype(jnp.bfloat16)
    low = (table - high.astype(np.float32)).astype(jnp.bfloat16)
    return high, low


def bits_of(number, count):
    return [number // 2**j % 2 for j in range(count.bit_length() - 1)]


def swapped(me, k, count):
    total = 0
    for j, bit in enumerate(bits_of(me, count)):
        total += ((1 - bit) if k >> j & 1 else bit) * 2**j
    return total


def flip(me, k, count):
    odd = 0
    for j, bit in enumerate(bits_of(me, count)):
        odd += 0 if k >> j & 1 else bit
    return 1.0 if isinstance(odd, int) else (1 - 2 * (odd % 2)).astype(jnp.float32)


def place(tok, row_count, width, window):
    first = tok * row_count
    owner = first // width
    offset = first - owner * width
    start = jnp.minimum(offset // LANES * LANES, width - window)
    return owner, start, offset - start


def window_size(groups, row_count, width):
    need = max(i * row_count % width % LANES + row_count for i in range(groups))
    return min(-(-need // LANES) * LANES, width)


def tile_size(width):
    return max(t for t in range(LANES, 513, LANES) if width % t == 0)


def remote(src, dst, send, arrive, to_tok, to_blk):
    return pltpu.make_async_remote_copy(
        src, dst, send, arrive, device_id={"tok": to_tok, "blk": to_blk}, device_id_type=MESH
    )


def greet(tok, blk, core, z, x, depth, across):
    blocks = lax.axis_size("blk")
    barrier = pltpu.get_barrier_semaphore()

    def signal(to_tok, to_blk):
        pl.semaphore_signal(barrier, inc=1, device_id={"tok": to_tok, "blk": to_blk}, device_id_type=MESH)

    twin = tok + 1 - 2 * core
    for k in range(1, blocks):
        other = swapped(blk, k, blocks)
        signal(tok, other)
        signal(twin, other)
    count = 2 * blocks - 1
    for place_, size, stride in ((x, across, 2), (z, depth, 2 * across)):
        for way in (1, -1):
            there = (place_ + way >= 0) & (place_ + way < size)
            count += there.astype(jnp.int32)

            @pl.when(there)
            def _():
                signal(tok + stride * way, blk)

    signal(twin, blk)
    pl.semaphore_wait(barrier, count)


def broadcast_start(tok, blk, src, dst, send, recv):
    tokens, blocks = lax.axis_size("tok"), lax.axis_size("blk")
    count = tokens * blocks
    me = tok * blocks + blk

    @pl.loop(1, count)
    def _(k):
        other = lax.rem(me + k, count)
        remote(src, dst.at[me], send, recv, other // blocks, other % blocks).start()


def broadcast_wait(tok, blk, dst, send, recv):
    count = lax.axis_size("tok") * lax.axis_size("blk") - 1
    both = remote(dst.at[pl.ds(0, count)], dst.at[pl.ds(0, count)], send, recv, tok, blk)
    both.wait_send()
    both.wait_recv()


def kernel(
    depth, across, sub, early, lag, row_count, x_ref, signs_ref, high_hbm, low_hbm,
    acc, notes, cols, rows, pieces, *rest,
):
    blocks, width = lax.axis_size("blk"), x_ref.shape[1]
    signs, rest = [ref.at[pl.ds(0, width)] for ref in rest[:blocks]], rest[blocks:]
    run(
        depth, across, sub, early, lag, row_count, x_ref, signs_ref, high_hbm, low_hbm,
        acc, notes, cols, rows, pieces, signs, *rest,
    )


def run(
    depth, across, sub, early, lag, row_count, x_ref, signs_ref, high_hbm, low_hbm,
    acc, notes, cols, rows, pieces, signs, high, low, lhs, left, square, best,
    table_sem, x_sem, sign_sem, sign_send, sign_recv, swap_send, swap_recv,
    recv, pair_send, pair_recv, z_send, x_send, y_send, y_recv, note_send, note_recv,
):
    tok, blk = lax.axis_index("tok"), lax.axis_index("blk")
    blocks, groups = lax.axis_size("blk"), lax.axis_size("tok")
    tok_rows, width = x_ref.shape
    window = rows.shape[1]
    half = cols.shape[0] // 2
    steps = tok_rows // sub
    chunks = width // UNIT
    core, chip = tok % 2, tok // 2
    z, x = chip // across, chip % across
    me = tok * blocks + blk
    owner, start, skew = place(tok, row_count, width, window)
    start = pl.multiple_of(start, LANES)

    loads = [
        pltpu.make_async_copy(high_hbm, high, table_sem.at[0]),
        pltpu.make_async_copy(low_hbm, low, table_sem.at[1]),
        pltpu.make_async_copy(x_ref, pieces.at[0], x_sem),
        pltpu.make_async_copy(signs_ref, signs[0], sign_sem),
    ]
    for load in loads:
        load.start()
    greet(tok, blk, core, z, x, depth, across)

    for k in range(1, blocks):
        remote(signs_ref, signs[k], sign_send, sign_recv.at[k], tok, swapped(blk, k, blocks)).start()

    @pl.loop(0, steps)
    def _(s):
        piece = pl.ds(pl.multiple_of(s * sub, sub), sub)
        for k in range(1, blocks):
            remote(
                x_ref.at[piece], pieces.at[k, piece], swap_send, swap_recv.at[k * steps + s],
                tok, swapped(blk, k, blocks),
            ).start()

    for load in loads:
        load.wait()
    for k in range(1, blocks):
        remote(signs[k], signs[k], sign_send, sign_recv.at[k], tok, blk).wait_recv()
    def first_row(oz, ox, s):
        return pl.multiple_of(((oz * across + ox) * 2 + core) * tok_rows + s * sub, sub)

    def rotate(s):
        piece = pl.ds(pl.multiple_of(s * sub, sub), sub)
        for k in range(1, blocks):
            landed = pieces.at[k, piece]
            remote(landed, landed, swap_send, swap_recv.at[k * steps + s], tok, blk).wait_recv()
        for k in range(blocks):
            for c in range(chunks):
                lanes = slice(c * UNIT, (c + 1) * UNIT)
                value = pieces[k, piece, lanes].astype(jnp.float32) * signs[k][lanes].reshape(1, UNIT)
                first = (k * chunks + c) * sub
                lhs[first : first + sub, :] = value.astype(jnp.bfloat16)
        value = jnp.dot(lhs[...], high[...], preferred_element_type=jnp.float32)
        value += jnp.dot(lhs[...], low[...], preferred_element_type=jnp.float32)
        mixed = []
        for c in range(chunks):
            total = None
            for k in range(blocks):
                first = (k * chunks + c) * sub
                part = value[first : first + sub] * flip(blk, k, blocks)
                total = part if total is None else total + part
            mixed.append(total)
        step = 1
        while step < chunks:
            for a in range(chunks):
                if not a & step:
                    p, q = mixed[a], mixed[a | step]
                    mixed[a], mixed[a | step] = p + q, p - q
            step *= 2
        row = first_row(z, x, s)
        total = square[...]
        for c in range(chunks):
            rounded = (mixed[c] * (1.0 / math.sqrt(WALSH))).astype(jnp.bfloat16)
            cols[pl.ds(row, sub), c * UNIT : (c + 1) * UNIT] = rounded
            wide = rounded.astype(jnp.float32)
            wide = wide * wide
            for i in range(0, sub, 8):
                for j in range(0, UNIT, LANES):
                    total += wide[i : i + 8, j : j + LANES]
        square[...] = total

    def fan(oz, ox, s, z_ways, x_ways):
        row = first_row(oz, ox, s)
        src = cols.at[pl.ds(row, sub)]
        arrive = recv.at[(oz * across + ox) * steps + s]
        for way in z_ways:

            @pl.when((z + way >= 0) & (z + way < depth))
            def _():
                remote(src, src, z_send.at[(way + 1) // 2], arrive, tok + 2 * across * way, blk).start()

        for way in x_ways:

            @pl.when((x + way >= 0) & (x + way < across))
            def _():
                remote(src, src, x_send.at[(way + 1) // 2], arrive, tok + 2 * way, blk).start()

        remote(src, src, pair_send, pair_recv.at[oz * across + ox], tok + 1 - 2 * core, blk).start()
        for j in range(2):
            j_owner, j_start, _ = place(chip * 2 + j, row_count, width, window)

            @pl.when(j_owner == blk)
            def _():
                part = cols.at[pl.ds(row, sub), pl.ds(pl.multiple_of(j_start, LANES), window)]
                for k in range(1, blocks):
                    remote(
                        part, rows.at[pl.ds(row, sub)], y_send.at[2 * k + j],
                        y_recv.at[oz * across + ox], chip * 2 + j, lax.rem(blk + k, blocks),
                    ).start()

    def relay(oz, ox, s, z_ways, x_ways):
        piece = cols.at[pl.ds(first_row(oz, ox, s), sub)]
        remote(piece, piece, pair_send, recv.at[(oz * across + ox) * steps + s], tok, blk).wait_recv()
        fan(oz, ox, s, z_ways, x_ways)

    def inside(oz, ox):
        return (oz >= 0) & (oz < depth) & (ox >= 0) & (ox < across)

    def along_z(d, s):
        for way in (1, -1):
            oz = z - way * d

            @pl.when(inside(oz, x) & (s >= early))
            def _():
                relay(oz, x, s, (way,), (1, -1))

            @pl.when(inside(oz, x) & (s < early))
            def _():
                relay(oz, x, s, (way,), ())

    def along_x(d, dx, s):
        for side in (1, -1) if d else (1,):
            oz = z - side * d
            for way in (1, -1):
                ox = x - way * dx

                @pl.when(inside(oz, ox))
                def _():
                    relay(oz, ox, s, (), (way,))

    def early_x(dx, s):
        for way in (1, -1):
            ox = x - way * dx

            @pl.when(inside(z, ox))
            def _():
                relay(z, ox, s, (1, -1), (way,))

    def extra_z(d):
        for way in (1, -1):
            oz = z - way * d
            for dx in range(1, across):
                for side in (1, -1):
                    ox = x - side * dx

                    @pl.when(inside(oz, ox))
                    def _():
                        for s in range(early):
                            relay(oz, ox, s, (way,), ())

    tile = tile_size(width)
    tiles = width // tile
    chunks_all = depth * across
    base = tok * row_count - blk * width - skew

    def chunk_at(q):
        k, ox = q // across, lax.rem(x + q % across, across)
        if depth == 1:
            return k, ox
        near = z < depth // 2
        edge = jnp.where(near, z, depth - 1 - z)
        oz = jnp.where(k == 0, edge, jnp.where(k == 1, 1 - edge, k))
        return jnp.where(near, oz, depth - 1 - oz), ox

    def gram_open(q):
        oz, ox = chunk_at(q)
        n = oz * across + ox
        chunk = pl.ds(pl.multiple_of(n * 2 * tok_rows, sub), 2 * tok_rows)
        piece = cols.at[pl.ds(0, tok_rows)]
        remote(piece, piece, pair_send, pair_recv.at[n], tok, blk).wait_recv()

        @pl.when(owner == blk)
        def _():
            left[...] = jnp.transpose(cols[chunk, pl.ds(start, window)])

        @pl.when(owner != blk)
        def _():
            piece = rows.at[pl.ds(0, 2 * tok_rows)]
            remote(piece, piece, pair_send, y_recv.at[n], tok, blk).wait_recv()
            left[...] = jnp.transpose(rows[chunk, :])

    def gram_tile(q, t, first, last):
        oz, ox = chunk_at(q)
        n = oz * across + ox
        chunk = pl.ds(pl.multiple_of(n * 2 * tok_rows, sub), 2 * tok_rows)
        lanes = pl.ds(pl.multiple_of(t * tile, tile), tile)
        block = jnp.dot(left[...], cols[chunk, lanes], preferred_element_type=jnp.float32)
        if not first:
            block += acc[:, lanes]
        acc[:, lanes] = block
        if last:
            row = lax.broadcasted_iota(jnp.int32, (window, tile), 0) + (base - t * tile)
            column = lax.broadcasted_iota(jnp.int32, (window, tile), 1)
            size = jnp.where(row == column, 0.0, jnp.abs(block))
            most = best[...]
            for j in range(0, tile, LANES):
                most = jnp.maximum(most, size[:, j : j + LANES])
            best[...] = most

    def gram_whole(q, first=False, last=False):
        gram_open(q)

        @pl.loop(0, tiles)
        def _(t):
            gram_tile(q, t, first, last)

    def gram_some(begin, count):
        @pl.loop(begin, begin + count)
        def _(g):
            q, t = g // tiles, g % tiles

            @pl.when(t == 0)
            def _():
                gram_open(q)

            gram_tile(q, t, False, False)

    square[...] = jnp.zeros_like(square)
    best[...] = jnp.zeros_like(best)

    @pl.loop(0, steps + lag)
    def _(s):
        @pl.when(s < steps)
        def _():
            rotate(s)
            fan(z, x, s, (1, -1), (1, -1))

        u = s - lag
        if depth > 1:

            @pl.when(u >= 0)
            def _():
                along_z(1, u)

        if across > 1:

            @pl.when((u >= 0) & (u < early))
            def _():
                for dx in range(1, across):
                    early_x(dx, u)

            @pl.when(u >= early)
            def _():
                along_x(0, 1, u)

    extra_z(1)
    gram_whole(0, first=True)
    done = tiles
    paced = across == 2 and depth == 4
    ready = {2: 3, 3: 5, 4: 7}
    for d in range(2, depth + 1):
        goal = ready[d] * tiles if paced else done
        per = -(-(goal - done) // steps)

        @pl.loop(0, steps)
        def _(s):
            if d < depth:
                along_z(d, s)
            if across > 1:

                @pl.when(s >= early)
                def _():
                    along_x(d - 1, 1, s)

            if paced:
                begin = jnp.minimum(done + s * per, goal)
                gram_some(begin, jnp.minimum(per, goal - begin))

        if d < depth:
            extra_z(d)
        done = goal

    for dx in range(2, across):
        for d in range(depth):

            @pl.loop(early, steps)
            def _(s):
                along_x(d, dx, s)

    gram_some(done, (chunks_all - 1) * tiles - done)
    gram_whole(chunks_all - 1, last=True)

    flat = jnp.max(jnp.transpose(best[...]), axis=0, keepdims=True)
    lane = lax.broadcasted_iota(jnp.int32, (1, window), 1)
    notes[me, :, :window] = jnp.where((lane >= skew) & (lane < skew + row_count), flat, 0.0)
    notes[me, :, window:] = jnp.sum(square[...], axis=0, keepdims=True)
    broadcast_start(tok, blk, notes.at[me], notes, note_send, note_recv)

    def settle(count, send):
        piece = cols.at[pl.ds(0, count)]
        remote(piece, piece, send, note_recv, tok, blk).wait_send()

    late = steps - early
    for v in range(depth):

        @pl.when(z == v)
        def _():
            unit = (late + early * across) * sub
            if v < depth - 1:
                settle((v + 1) * unit, z_send.at[1])
            if v > 0:
                settle((depth - v) * unit, z_send.at[0])

    for v in range(across):

        @pl.when(x == v)
        def _():
            unit = (late * depth + early) * sub
            if v < across - 1:
                settle((v + 1) * unit, x_send.at[1])
            if v > 0:
                settle((across - v) * unit, x_send.at[0])

    settle(half, pair_send)
    for j in range(2):
        j_owner, _, _ = place(chip * 2 + j, row_count, width, window)

        @pl.when(j_owner == blk)
        def _():
            piece = rows.at[pl.ds(0, half)]
            for k in range(1, blocks):
                remote(piece, piece, y_send.at[2 * k + j], note_recv, tok, blk).wait_send()

    for k in range(1, blocks):
        remote(signs[k], signs[k], sign_send, note_recv, tok, blk).wait_send()
    if blocks > 1:
        sent = pieces.at[pl.ds(0, blocks - 1)]
        remote(sent, sent, swap_send, note_recv, tok, blk).wait_send()

    broadcast_wait(tok, blk, notes, note_send, note_recv)


def finish_kernel(row_count, lines, acc, notes, hess_ref, ratio_ref, top_ref, scaled, sems):
    tok, blk = lax.axis_index("tok"), lax.axis_index("blk")
    blocks, groups = lax.axis_size("blk"), lax.axis_size("tok")
    window, width = acc.shape
    _, _, skew = place(tok, row_count, width, window)
    total, most = notes[0, :, window:], notes[0, :, :window]
    for i in range(1, groups * blocks):
        total += notes[i, :, window:]
        most = jnp.maximum(most, notes[i, :, :window])
    inverse = 1.0 / (jnp.sum(total, keepdims=True) / FEATURES + EPS)

    def out(r):
        piece = pl.ds(pl.multiple_of(r * lines, 8), lines)
        return pltpu.make_async_copy(scaled.at[piece], hess_ref.at[piece], sems.at[r])

    @pl.loop(0, row_count // lines)
    def _(r):
        row = lax.broadcasted_iota(jnp.int32, (lines, width), 0) + (tok * row_count - blk * width + r * lines)
        column = lax.broadcasted_iota(jnp.int32, (lines, width), 1)
        block = acc[pl.ds(pl.multiple_of(skew + r * lines, 8), lines), :] * inverse
        scaled[pl.ds(pl.multiple_of(r * lines, 8), lines), :] = block + jnp.where(row == column, DAMP, 0.0)
        out(r).start()

    top_ref[...] = jnp.max(most, keepdims=True) * inverse
    for b in range(blocks):

        @pl.when(blk == b)
        def _():
            whole = [None] * (width // LANES)
            for i in range(groups):
                first = i * row_count
                if first // width == b:
                    offset = first % width
                    begin = min(offset // LANES * LANES, width - window) // LANES
                    for j in range(window // LANES):
                        for k in range(blocks):
                            value = notes[i * blocks + k, :, j * LANES : (j + 1) * LANES]
                            old = whole[begin + j]
                            whole[begin + j] = value if old is None else jnp.maximum(old, value)
            ratio_ref[...] = (jnp.concatenate(whole, axis=1) * inverse).reshape(width)

    @pl.loop(0, row_count // lines)
    def _(r):
        out(r).wait()


def per_device(activations, signs):
    tok_rows, width = activations.shape
    groups, blocks = lax.axis_size("tok"), lax.axis_size("blk")
    depth = 4 if groups % 8 == 0 else 1
    across = groups // (2 * depth)
    sub, early, lag = 16, 1, 3
    steps = tok_rows // sub
    row_count = FEATURES // groups
    window = window_size(groups, row_count, width)
    count, chips, tokens = groups * blocks, groups // 2, groups * tok_rows
    lines = max(t for t in range(8, 65, 8) if row_count % t == 0)
    high, low = unit_tables()
    dma = pltpu.SemaphoreType.DMA
    hbm = pl.BlockSpec(memory_space=pltpu.HBM)
    vmem = pl.BlockSpec(memory_space=pltpu.VMEM)
    gram, notes = pl.pallas_call(
        functools.partial(kernel, depth, across, sub, early, lag, row_count),
        out_shape=(
            jax.ShapeDtypeStruct((window, width), jnp.float32),
            jax.ShapeDtypeStruct((count + 1, 1, window + LANES), jnp.float32),
        ),
        in_specs=[hbm] * 4,
        out_specs=(vmem, vmem),
        scratch_shapes=[
            pltpu.VMEM((tokens, width), jnp.bfloat16),
            pltpu.VMEM((tokens, window), jnp.bfloat16),
            pltpu.VMEM((blocks, tok_rows, width), jnp.bfloat16),
        ]
        + [pltpu.VMEM((width + 1024,), jnp.float32)] * blocks
        + [
            pltpu.VMEM((UNIT, UNIT), jnp.bfloat16),
            pltpu.VMEM((UNIT, UNIT), jnp.bfloat16),
            pltpu.VMEM((blocks * (width // UNIT) * sub, UNIT), jnp.bfloat16),
            pltpu.VMEM((window, 2 * tok_rows), jnp.bfloat16),
            pltpu.VMEM((8, LANES), jnp.float32),
            pltpu.VMEM((window, LANES), jnp.float32),
            dma((2,)), dma, dma, dma, dma((blocks,)), dma, dma((blocks * steps,)),
            dma((chips * steps,)), dma, dma((chips,)), dma((2,)), dma((2,)), dma((2 * blocks,)), dma((chips,)),
            dma, dma,
        ],
        compiler_params=pltpu.CompilerParams(
            collective_id=0, has_side_effects=True, vmem_limit_bytes=36 * 1024 * 1024
        ),
        name="fused",
    )(activations, signs, jnp.asarray(high), jnp.asarray(low))
    hessian, ratio, top = pl.pallas_call(
        functools.partial(finish_kernel, row_count, lines),
        out_shape=(
            jax.ShapeDtypeStruct((row_count, width), jnp.float32),
            jax.ShapeDtypeStruct((width,), jnp.float32),
            jax.ShapeDtypeStruct((1, 1), jnp.float32),
        ),
        in_specs=[vmem, vmem],
        out_specs=(hbm, vmem, vmem),
        scratch_shapes=[pltpu.VMEM((row_count, width), jnp.float32), dma((row_count // lines,))],
        compiler_params=pltpu.CompilerParams(vmem_limit_bytes=24 * 1024 * 1024),
        name="finish",
    )(gram, notes)
    return hessian, ratio, top.reshape(())


def solution(mesh):
    in_specs = (P("tok", "blk"), P("blk"))
    out_specs = (P("tok", "blk"), P("blk"), P())
    return jax.shard_map(
        per_device, mesh=mesh, in_specs=in_specs, out_specs=out_specs, check_vma=False
    )
```
